32 devices in a mesh: row: 4 (over y, x), col: 8 (over z, core).
Axes of the slice: x: 2, y: 2, z: 4, core: 2. Of those that a mesh axis runs over, the one named last changes fastest.
Arguments:
- panel: float32 [12288, 512], P(('row', 'col')), may hold values from -0.054126588 to 0.054126588
- trailing: float32 [12288, 4096], P('row', 'col'), may hold values from -6 to 6
- counts: int32 [4], P('row'), may hold values from 1 to 6, 14 in all
Outputs:
- upper: float32 [512, 512], replicated
- projected: float32 [512, 4096], P(None, 'col')
The draws below stay inside these ranges and needn't reach their ends.
Inputs may be any that keep to these rules, and one draw needn't show every extreme that they name: `counts`: the valid tiles of a block are its first ones; some grid row has all 6 valid.
All inputs are finite; a program needn't handle non-finite values.
Results may differ from the reference program's by a relative error of at most 0.0003.
Values sent between devices are 32-bit elements; how exact they have to be, the bound alone decides.
A program may use at most 64 MiB of HBM per device.

```python
import math
import jax
import jax.numpy as jnp
import numpy as np
from jax import lax

B = 512
TILES_DEV = 6
ROWS = 12288
NC = 4096
N_ROW = 4


def draw_panel(key, part):
    base = jax.random.fold_in(key, 11)
    key_own, key_shared = jax.random.split(base, 2)
    share = 0.02
    own = jax.random.normal(key_own, (ROWS, B), jnp.float32)
    shared = jax.random.normal(key_shared, (ROWS, 1), jnp.float32)
    values = math.sqrt(1.0 - share) * own + math.sqrt(share) * shared
    values = jnp.clip(values, -6.0, 6.0) * float(ROWS) ** (-0.5)
    return values.astype(jnp.float32)


def levels(rng, shape, shards, low, largest):
    def one(axis_at, shards_of):
        draws = jax.random.uniform(jax.random.fold_in(jax.random.fold_in(rng, 6), axis_at), (shards_of,), jnp.float32, low / len(shards), largest / len(shards))
        return jnp.repeat(jnp.exp(draws), shape[axis_at] // shards_of).reshape((-1,) + (1,) * (len(shape) - axis_at - 1))

    loudness = one(*shards[0])
    for cut in shards[1:]:
        loudness = loudness * one(*cut)
    return loudness


def length_profile(number_of, total, limit, slope):
    weights = [(1 << 20) // math.isqrt(grade ** slope) + 1 for grade in range(2, number_of + 1)]
    rest, given = total - limit - (number_of - 1), [1] * (number_of - 1)
    while rest > 0:
        free = [i for i in range(number_of - 1) if given[i] < limit]
        whole, remaining = sum([weights[i] for i in free]), rest
        for i in free:
            extra = min(limit - given[i], max(1, remaining * weights[i] // whole), rest)
            given[i] = given[i] + extra
            rest = rest - extra
    return np.array([limit] + given)


def uneven_parts(key, number_of, total, bound, skew):
    if number_of == 2:
        one = jax.random.randint(key, (), max(1, total - bound), min(bound, total - 1) + 1)
        return jnp.stack([one, total - one])
    tallies = jnp.asarray(length_profile(number_of, total, bound, skew), jnp.int32)
    couples = (number_of - 1) // 2
    donor, receiver = tallies[1:1 + 2 * couples:2], tallies[2:2 + 2 * couples:2]
    room = jnp.minimum(donor - 1, bound - receiver)
    passed = jax.random.randint(jax.random.fold_in(key, 1), (couples,), 0, 1 << 20) % (room + 1)
    tallies = tallies.at[1:1 + 2 * couples:2].set(donor - passed).at[2:2 + 2 * couples:2].set(receiver + passed)
    return tallies[jax.random.permutation(jax.random.fold_in(key, 2), number_of)]


def centred(own_key, extent, scale, reach, shards=(), held_as=jnp.bfloat16):
    factor_of = levels(own_key, extent, shards, -0.22, 0.18) if shards else 1.0
    array = jax.random.normal(own_key, extent, jnp.float32) * scale * factor_of
    return jnp.minimum(jnp.maximum(array, -reach), reach).astype(held_as)


def setup_inputs(seed: int = 0) -> dict:
    seeds = jax.random.split(jax.random.key(seed), 4)
    panel = draw_panel(jax.random.fold_in(seeds[3], 71), 0)
    trailing = centred(seeds[1], (ROWS, NC), 1.0, 6.0, ((0, 4), (1, 8)), jnp.float32)
    counts = uneven_parts(seeds[2], N_ROW, (TILES_DEV + 1) * N_ROW // 2, TILES_DEV, 0).astype(jnp.int32)
    return {"panel": panel, "trailing": trailing, "counts": counts}


def reference(panel, trailing, counts):
    width = panel.shape[1]
    indices = lax.iota(jnp.int32, ROWS)
    block = indices // (TILES_DEV * width)
    tile = indices % (TILES_DEV * width) // width
    keep = (tile < counts[block]).astype(jnp.float32)
    masked = panel * keep[:, None]
    factor_q, factor_r = jnp.linalg.qr(masked)
    signs = jnp.sign(jnp.diagonal(factor_r))
    upper = signs[:, None] * factor_r
    projected = signs[:, None] * jnp.dot(factor_q.T.astype(jnp.float32), trailing.astype(jnp.float32), precision=lax.Precision.HIGHEST, preferred_element_type=jnp.float32)
    return (upper, projected)
```

```python
import functools

import jax
import jax.numpy as jnp
from jax import lax
from jax.experimental import pallas as pl
from jax.experimental.pallas import tpu as pltpu
from jax.sharding import PartitionSpec as P

MESH = pl.DeviceIdType.MESH
LANES = 128
GROUP = 8


def split(x):
    high = x.astype(jnp.bfloat16)
    return high, (x - high.astype(jnp.float32)).astype(jnp.bfloat16)


def dot3(left, right, dims):
    one = functools.partial(
        lax.dot_general, dimension_numbers=(dims, ((), ())), preferred_element_type=jnp.float32
    )
    return one(left[0], right[0]) + (one(left[0], right[1]) + one(left[1], right[0]))


def bits_of(axis, size):
    return [(axis, 1 << b) for b in range(size.bit_length() - 1)]


def plan(rows, order):
    steps = []
    for axis, bit in order:
        halve = rows % (2 * GROUP) == 0
        steps.append((axis, bit, rows, halve))
        rows = rows // 2 if halve else rows
    return steps


def partner(axis, bit):
    me = lax.axis_index(axis)
    mine = lax.rem(me // bit, 2)
    return mine, {axis: me + bit - 2 * bit * mine}


def greet(axis_bits):
    barrier = pltpu.get_barrier_semaphore()
    for axis, bit in axis_bits:
        _, other = partner(axis, bit)
        pl.semaphore_signal(barrier, inc=1, device_id=other, device_id_type=MESH)
    pl.semaphore_wait(barrier, len(axis_bits))


def reduce_all(acc, out, landing, send, recv, streams):
    count = len(streams[0][1])
    offsets = [[start] for start, _ in streams]

    def copy(n, src, dst, other):
        return pltpu.make_async_remote_copy(
            src_ref=src, dst_ref=dst, send_sem=send.at[n], recv_sem=recv.at[n],
            device_id=other, device_id_type=MESH,
        )

    pending = []
    slot = 0
    for s in range(count):
        copies = []
        for i, (_, steps) in enumerate(streams):
            axis, bit, rows, halve = steps[s]
            mine, other = partner(axis, bit)
            at = offsets[i][-1]
            size = rows // 2 if halve else rows
            keep = at + mine * size if halve else at
            away = at + (1 - mine) * size if halve else at
            keep, away = pl.multiple_of(keep, GROUP), pl.multiple_of(away, GROUP)
            land = landing.at[pl.ds(slot, size)]
            c = copy(2 * len(streams) * s + i, acc.at[pl.ds(away, size)], land, other)
            c.start()
            copies.append((c, keep, size, slot, halve))
            offsets[i].append(keep)
            slot += size
        for c, keep, size, here, halve in copies:
            if halve:
                c.wait_recv()
                pending.append(c)
            else:
                c.wait()
            target = out if s == count - 1 else acc
            target[pl.ds(keep, size)] = acc[pl.ds(keep, size)] + landing[pl.ds(here, size)]
    for c in pending:
        c.wait_send()
    pending = []
    for s in reversed(range(count)):
        copies = []
        for i, (_, steps) in enumerate(streams):
            axis, bit, rows, halve = steps[s]
            if not halve:
                continue
            _, other = partner(axis, bit)
            size = rows // 2
            region = out.at[pl.ds(offsets[i][s + 1], size)]
            c = copy(2 * len(streams) * s + len(streams) + i, region, region, other)
            c.start()
            copies.append(c)
        for c in copies:
            c.wait_recv()
        pending += copies
    for c in pending:
        c.wait_send()


def landing_rows(streams):
    return sum(r // 2 if h else r for _, steps in streams for _, _, r, h in steps)


def blocks_of(width):
    tiles = width // LANES
    return [(i, j) for i in range(tiles) for j in range(i, tiles)]


def gram_kernel(streams, order, piece_ref, out_ref, acc, landing, send, recv):
    high, low = split(piece_ref[...])
    for n, (i, j) in enumerate(blocks_of(piece_ref.shape[1])):
        a, b = slice(i * LANES, (i + 1) * LANES), slice(j * LANES, (j + 1) * LANES)
        acc[n * LANES:(n + 1) * LANES] = dot3(
            (high[:, a], low[:, a]), (high[:, b], low[:, b]), ((0,), (0,))
        )
    greet(order)
    reduce_all(acc, out_ref, landing, send, recv, streams)


def sum_kernel(streams, order, in_ref, out_ref, acc, landing, send, recv):
    acc[...] = in_ref[...]
    greet(order)
    reduce_all(acc, out_ref, landing, send, recv, streams)


def two_streams(rows, first, second):
    half = rows // 2
    return [(0, plan(half, first)), (half, plan(half, second))]


def call_reducing(kernel, value, rows, lanes, streams, order, ident):
    copies = 2 * len(streams) * len(streams[0][1])
    return pl.pallas_call(
        functools.partial(kernel, streams, order),
        out_shape=jax.ShapeDtypeStruct((rows, lanes), jnp.float32),
        in_specs=[pl.BlockSpec(memory_space=pltpu.VMEM)],
        out_specs=pl.BlockSpec(memory_space=pltpu.VMEM),
        scratch_shapes=[
            pltpu.VMEM((rows, lanes), jnp.float32),
            pltpu.VMEM((landing_rows(streams), lanes), jnp.float32),
            pltpu.SemaphoreType.DMA((copies,)),
            pltpu.SemaphoreType.DMA((copies,)),
        ],
        compiler_params=pltpu.CompilerParams(collective_id=ident, has_side_effects=True),
        cost_estimate=pl.CostEstimate(flops=10**9, bytes_accessed=2 * 10**7, transcendentals=0),
    )(value)


def factor_group(work, g):
    at = g * GROUP
    left = work[at:at + GROUP, :LANES]
    right = work[at:at + GROUP, LANES:]
    rows = lax.broadcasted_iota(jnp.int32, (GROUP, LANES), 0)
    columns = [
        jnp.broadcast_to(left[:, at + j:at + j + 1], (GROUP, LANES)) for j in range(GROUP)
    ]
    for j in range(GROUP):
        scale = lax.rsqrt(columns[j][j:j + 1, :])
        factor = columns[j] * scale
        below = jnp.where(rows > j, factor, 0.0)
        left_j, right_j = left[j:j + 1, :] * scale, right[j:j + 1, :] * scale
        left = jnp.where(rows == j, left_j, left - below * left_j)
        right = jnp.where(rows == j, right_j, right - below * right_j)
        for k in range(j + 1, GROUP):
            columns[k] = columns[k] - below * factor[k:k + 1, :]
    work[at:at + GROUP, :LANES] = left
    work[at:at + GROUP, LANES:] = right
    rest = LANES - at - GROUP
    if rest:
        high, low = split(jnp.concatenate([left, right], axis=1))
        shift = (high[:, at + GROUP:LANES], low[:, at + GROUP:LANES])
        work[at + GROUP:] = work[at + GROUP:] - dot3(shift, (high, low), ((0,), (0,)))


def factor_kernel(packed_ref, upper_ref, inverse_ref, whole, work):
    width = upper_ref.shape[0]
    whole[...] = jnp.zeros_like(whole)
    for n, (i, j) in enumerate(blocks_of(width)):
        whole[i * LANES:(i + 1) * LANES, j * LANES:(j + 1) * LANES] = packed_ref[
            n * LANES:(n + 1) * LANES
        ]
    square = lax.broadcasted_iota(jnp.int32, (LANES, LANES), 0)
    across = lax.broadcasted_iota(jnp.int32, (LANES, LANES), 1)
    unit = (square == across).astype(jnp.float32)
    for t in range(width // LANES):
        a, b = t * LANES, (t + 1) * LANES
        whole[a:b, width + a:width + b] = unit

    for t in range(width // LANES):
        a, b = t * LANES, (t + 1) * LANES
        work[:, :LANES] = whole[a:b, a:b]
        work[:, LANES:] = unit
        for g in range(LANES // GROUP):
            factor_group(work, g)
        inverse = split(work[:, LANES:])
        row = dot3(inverse, split(whole[a:b, a:width + b]), ((1,), (0,)))
        whole[a:b, a:width + b] = row
        whole[a:b, a:b] = jnp.where(across >= square, work[:, :LANES], 0.0)
        if t:
            whole[a:b, :a] = jnp.zeros((LANES, a), jnp.float32)
        if b < width:
            high, low = split(row)
            rest = width - b
            shift = (high[:, LANES:LANES + rest], low[:, LANES:LANES + rest])
            tail = (high[:, LANES:], low[:, LANES:])
            whole[b:, b:width + b] = whole[b:, b:width + b] - dot3(shift, tail, ((0,), (0,)))
    upper_ref[...] = whole[:, :width]
    inverse_ref[...] = whole[:, width:]


def factorize(packed, width):
    square = jax.ShapeDtypeStruct((width, width), jnp.float32)
    return pl.pallas_call(
        factor_kernel,
        out_shape=(square, square),
        in_specs=[pl.BlockSpec(memory_space=pltpu.VMEM)],
        out_specs=[pl.BlockSpec(memory_space=pltpu.VMEM)] * 2,
        scratch_shapes=[
            pltpu.VMEM((width, 2 * width), jnp.float32),
            pltpu.VMEM((LANES, 2 * LANES), jnp.float32),
        ],
        cost_estimate=pl.CostEstimate(flops=10**9, bytes_accessed=10**8, transcendentals=0),
    )(packed)


def body(n_row, n_col, panel, trailing, counts):
    width = panel.shape[1]
    valid = counts[0]
    piece = lax.all_gather(panel, "col", axis=0, tiled=True)

    own = lax.axis_index("col") * panel.shape[0] + lax.iota(jnp.int32, panel.shape[0])
    masked = jnp.where((own // width < valid)[:, None], panel, 0.0)
    rows, columns = bits_of("row", n_row), bits_of("col", n_col)
    turned = rows[len(rows) // 2:] + rows[:len(rows) // 2]
    order = columns[:1] + rows + columns[1:]
    packed_rows = len(blocks_of(width)) * LANES
    packed = call_reducing(
        gram_kernel, masked, packed_rows, LANES,
        two_streams(packed_rows, order, columns[:1] + turned + columns[1:]), order, 0,
    )
    upper, inverse = factorize(packed, width)

    indices = lax.iota(jnp.int32, piece.shape[0])
    piece = jnp.where((indices // width < valid)[:, None], piece, 0.0)
    cross = lax.dot_general(
        piece, trailing, (((0,), (0,)), ((), ())),
        precision=lax.Precision.HIGH, preferred_element_type=jnp.float32,
    )
    cross = call_reducing(
        sum_kernel, cross, width, cross.shape[1], two_streams(width, rows, turned), rows, 1
    )
    projected = lax.dot(
        inverse, cross, precision=lax.Precision.HIGH, preferred_element_type=jnp.float32
    )
    return (upper, projected)


def solution(mesh):
    return jax.shard_map(
        functools.partial(body, mesh.shape["row"], mesh.shape["col"]),
        mesh=mesh,
        in_specs=(P(("row", "col"), None), P("row", "col"), P("row")),
        out_specs=(P(), P(None, "col")),
        check_vma=False,
    )
```

```python
import functools

import jax
import jax.numpy as jnp
from jax import lax
from jax.experimental import pallas as pl
from jax.experimental.pallas import tpu as pltpu
from jax.sharding import PartitionSpec as P

MESH = pl.DeviceIdType.MESH
LANES = 128
GROUP = 8
CORES = 2
HALVES = 2


def split(x):
    high = x.astype(jnp.bfloat16)
    return high, (x - high.astype(jnp.float32)).astype(jnp.bfloat16)


def dot3(left, right, dims):
    one = functools.partial(
        lax.dot_general, dimension_numbers=(dims, ((), ())), preferred_element_type=jnp.float32
    )
    return one(left[0], right[0]) + (one(left[0], right[1]) + one(left[1], right[0]))


def bits_of(axis, size):
    return [(axis, 1 << b) for b in range(size.bit_length() - 1)]


def plan(rows, order):
    steps = []
    for axis, bit in order:
        halve = rows % (2 * GROUP) == 0
        steps.append((axis, bit, rows, halve))
        rows = rows // 2 if halve else rows
    return steps


def partner(axis, bit):
    me = lax.axis_index(axis)
    mine = lax.rem(me // bit, 2)
    return mine, {axis: me + bit - 2 * bit * mine}


def nothing():
    pass


def reduce_all(acc, out, landing, send, recv, streams, hooks={}):
    count = len(streams[0][1])
    offsets = [[start] for start, _ in streams]

    def copy(n, src, dst, other):
        return pltpu.make_async_remote_copy(
            src_ref=src, dst_ref=dst, send_sem=send.at[n], recv_sem=recv.at[n],
            device_id=other, device_id_type=MESH,
        )

    pending = []
    slot = 0
    for s in range(count):
        copies = []
        for i, (_, steps) in enumerate(streams):
            axis, bit, rows, halve = steps[s]
            mine, other = partner(axis, bit)
            at = offsets[i][-1]
            size = rows // 2 if halve else rows
            keep = at + mine * size if halve else at
            away = at + (1 - mine) * size if halve else at
            keep, away = pl.multiple_of(keep, GROUP), pl.multiple_of(away, GROUP)
            land = landing.at[pl.ds(slot, size)]
            c = copy(2 * len(streams) * s + i, acc.at[pl.ds(away, size)], land, other)
            c.start()
            copies.append((c, keep, size, slot, halve))
            offsets[i].append(keep)
            slot += size
        hooks.get(("fold", s), nothing)()
        for c, keep, size, here, halve in copies:
            if halve:
                c.wait_recv()
                pending.append(c)
            else:
                c.wait()
            target = out if s == count - 1 else acc
            target[pl.ds(keep, size)] = acc[pl.ds(keep, size)] + landing[pl.ds(here, size)]
    for c in pending:
        c.wait_send()
    pending = []
    for s in reversed(range(count)):
        copies = []
        for i, (_, steps) in enumerate(streams):
            axis, bit, rows, halve = steps[s]
            if not halve:
                continue
            _, other = partner(axis, bit)
            size = rows // 2
            region = out.at[pl.ds(offsets[i][s + 1], size)]
            c = copy(2 * len(streams) * s + len(streams) + i, region, region, other)
            c.start()
            copies.append(c)
        hooks.get(("spread", s), nothing)()
        for c in copies:
            c.wait_recv()
        pending += copies
    for c in pending:
        c.wait_send()


def landing_rows(streams):
    return sum(r // 2 if h else r for _, steps in streams for _, _, r, h in steps)


def blocks_of(width):
    tiles = width // LANES
    return [(i, j) for i in range(tiles) for j in range(i, tiles)]


def two_streams(rows, first, second):
    half = rows // 2
    return [(0, plan(half, first)), (half, plan(half, second))]


def factor_group(work, g):
    at = g * GROUP
    left = work[at:at + GROUP, :LANES]
    right = work[at:at + GROUP, LANES:]
    rows = lax.broadcasted_iota(jnp.int32, (GROUP, LANES), 0)
    columns = [
        jnp.broadcast_to(left[:, at + j:at + j + 1], (GROUP, LANES)) for j in range(GROUP)
    ]
    for j in range(GROUP):
        scale = lax.rsqrt(columns[j][j:j + 1, :])
        factor = columns[j] * scale
        below = jnp.where(rows > j, factor, 0.0)
        left_j, right_j = left[j:j + 1, :] * scale, right[j:j + 1, :] * scale
        left = jnp.where(rows == j, left_j, left - below * left_j)
        right = jnp.where(rows == j, right_j, right - below * right_j)
        for k in range(j + 1, GROUP):
            columns[k] = columns[k] - below * factor[k:k + 1, :]
    work[at:at + GROUP, :LANES] = left
    work[at:at + GROUP, LANES:] = right
    rest = LANES - at - GROUP
    if rest:
        high, low = split(jnp.concatenate([left, right], axis=1))
        shift = (high[:, at + GROUP:LANES], low[:, at + GROUP:LANES])
        work[at + GROUP:] = work[at + GROUP:] - dot3(shift, (high, low), ((0,), (0,)))


def kernel(
    n_row, n_col, counts_ref, panel_ref, trailing_hbm, upper_ref, out_ref,
    pack, packed, pack_land, send, recv, gathered, trailing, total, summed, land, send2, recv2,
    whole, work, load, right_s, left_s, mate_s, line_r, mate_r,
):
    width = panel_ref.shape[1]
    rows_dev = panel_ref.shape[0]
    half = rows_dev // HALVES
    lines = n_col // CORES
    col = lax.axis_index("col")
    z, core = col // CORES, lax.rem(col, CORES)
    row_bits, col_bits = bits_of("row", n_row), bits_of("col", n_col)
    turned = row_bits[len(row_bits) // 2:] + row_bits[:len(row_bits) // 2]
    order = col_bits[:1] + row_bits + col_bits[1:]
    other_order = col_bits[:1] + turned + col_bits[1:]
    fold_streams = two_streams(packed.shape[0], order, other_order)
    sum_streams = two_streams(width, row_bits, turned)

    fetch = pltpu.make_async_copy(trailing_hbm, trailing, load)
    fetch.start()

    def place(src, h):
        at = (src * CORES + core) * rows_dev + h * half
        return gathered.at[pl.ds(pl.multiple_of(at, GROUP), half)]

    def send_copy(src, h, origin, sems, to):
        return pltpu.make_async_remote_copy(
            src_ref=origin, dst_ref=place(src, h), send_sem=sems.at[src * HALVES + h],
            recv_sem=line_r.at[src * HALVES + h], device_id={"col": to}, device_id_type=MESH,
        )

    def mate_copy(src, h, origin):
        return pltpu.make_async_remote_copy(
            src_ref=origin, dst_ref=place(src, h), send_sem=mate_s.at[src * HALVES + h],
            recv_sem=mate_r.at[src * HALVES + h], device_id={"col": col + 1 - 2 * core},
            device_id_type=MESH,
        )

    def start_own(h):
        origin = panel_ref.at[pl.ds(h * half, half)]

        @pl.when(z < lines - 1)
        def _():
            send_copy(z, h, origin, right_s, col + CORES).start()

        @pl.when(z > 0)
        def _():
            send_copy(z, h, origin, left_s, col - CORES).start()

        mate_copy(z, h, origin).start()

    def relay(s, h):
        @pl.when(z >= s)
        def _():
            src = z - s
            send_copy(src, h, place(src, h), right_s, col).wait_recv()

            @pl.when(z < lines - 1)
            def _():
                send_copy(src, h, place(src, h), right_s, col + CORES).start()

            mate_copy(src, h, place(src, h)).start()

        @pl.when(z + s < lines)
        def _():
            src = z + s
            send_copy(src, h, place(src, h), left_s, col).wait_recv()

            @pl.when(z > 0)
            def _():
                send_copy(src, h, place(src, h), left_s, col - CORES).start()

            mate_copy(src, h, place(src, h)).start()

    limit = counts_ref[0] * width

    def multiply(src):
        rows = CORES * rows_dev
        at = pl.multiple_of(src * rows, GROUP)
        index = at + lax.broadcasted_iota(jnp.int32, (rows, LANES), 0)
        right = split(trailing[pl.ds(at, rows)])
        for t in range(width // LANES):
            a, b = t * LANES, (t + 1) * LANES
            block = gathered[pl.ds(at, rows), a:b]
            left = split(jnp.where(index < limit, block, 0.0))
            total[a:b] = total[a:b] + dot3(left, right, ((0,), (0,)))

    def wait_mate(src):
        for h in range(HALVES):
            mate_copy(src, h, place(src, h)).wait_recv()

    def multiply_far(s):
        def one(d, carry):
            src = z - s + 2 * s * d

            @pl.when((src >= 0) & (src < lines))
            def _():
                wait_mate(src)
                multiply(src)

            return carry

        lax.fori_loop(0, 2, one, 0)

    barrier = pltpu.get_barrier_semaphore()
    for axis, bit in order:
        _, other = partner(axis, bit)
        pl.semaphore_signal(barrier, inc=1, device_id=other, device_id_type=MESH)

    for shift in (1, lines - 1):
        other = lax.rem(z + shift, lines) * CORES + core
        pl.semaphore_signal(barrier, inc=1, device_id={"col": other}, device_id_type=MESH)
    pl.semaphore_wait(barrier, len(order) + 2)

    start_own(0)
    first = col * rows_dev
    index = first + lax.broadcasted_iota(jnp.int32, (rows_dev, width), 0)
    high, low = split(jnp.where(index < limit, panel_ref[...], 0.0))
    for n, (i, j) in enumerate(blocks_of(width)):
        a, b = slice(i * LANES, (i + 1) * LANES), slice(j * LANES, (j + 1) * LANES)
        pack[n * LANES:(n + 1) * LANES] = dot3(
            (high[:, a], low[:, a]), (high[:, b], low[:, b]), ((0,), (0,))
        )

    polls = [(s, h) for s in range(1, lines) for h in range(HALVES)]
    last_z = len(row_bits) + 1

    def after_lines():
        for h in range(1, HALVES):
            start_own(h)
        relay(*polls[0])

    def own_product():
        total[...] = jnp.zeros_like(total)
        gathered[pl.ds(pl.multiple_of(first, GROUP), rows_dev)] = panel_ref[...]
        fetch.wait()
        wait_mate(z)
        multiply(z)

    reduce_all(
        pack, packed, pack_land, send, recv, fold_streams,
        {("spread", last_z): after_lines, ("spread", last_z - 1): own_product},
    )

    whole[...] = jnp.zeros_like(whole)
    for n, (i, j) in enumerate(blocks_of(width)):
        whole[i * LANES:(i + 1) * LANES, j * LANES:(j + 1) * LANES] = packed[
            n * LANES:(n + 1) * LANES
        ]
    square = lax.broadcasted_iota(jnp.int32, (LANES, LANES), 0)
    across = lax.broadcasted_iota(jnp.int32, (LANES, LANES), 1)
    unit = (square == across).astype(jnp.float32)
    for t in range(width // LANES):
        a, b = t * LANES, (t + 1) * LANES
        whole[a:b, width + a:width + b] = unit

    waiting = polls[1:]
    tiles = width // LANES
    done = 0
    relay(*waiting[0])
    passed = 1
    for t in range(tiles):
        a, b = t * LANES, (t + 1) * LANES
        work[:, :LANES] = whole[a:b, a:b]
        work[:, LANES:] = unit
        for g in range(LANES // GROUP):
            factor_group(work, g)
        inverse = split(work[:, LANES:])
        row = dot3(inverse, split(whole[a:b, a:width + b]), ((1,), (0,)))
        whole[a:b, a:width + b] = row
        whole[a:b, a:b] = jnp.where(across >= square, work[:, :LANES], 0.0)
        if t:
            whole[a:b, :a] = jnp.zeros((LANES, a), jnp.float32)
        if b < width:
            high, low = split(row)
            rest = width - b
            shift = (high[:, LANES:LANES + rest], low[:, LANES:LANES + rest])
            tail = (high[:, LANES:], low[:, LANES:])
            whole[b:, b:width + b] = whole[b:, b:width + b] - dot3(shift, tail, ((0,), (0,)))
        until = len(waiting) if t == tiles - 1 else 1 + (len(waiting) - 1) * (t + 1) // tiles
        while passed < until:
            relay(*waiting[passed])
            passed += 1
        complete = (passed + 1) // HALVES if t == tiles - 1 else passed // HALVES
        while done < complete:
            done += 1
            multiply_far(done)
    upper_ref[...] = whole[:, :width]

    reduce_all(total, summed, land, send2, recv2, sum_streams)
    inverse = split(whole[:, width:])
    out_ref[...] = dot3(inverse, split(summed[...]), ((1,), (0,)))

    for h in range(HALVES):
        mate_copy(z, h, place(z, h)).wait_send()

        @pl.when(z < lines - 1)
        def _():
            send_copy(z, h, place(z, h), right_s, col).wait_send()

        @pl.when(z > 0)
        def _():
            send_copy(z, h, place(z, h), left_s, col).wait_send()

    for s, h in polls:
        @pl.when(z >= s)
        def _():
            mate_copy(z - s, h, place(z - s, h)).wait_send()

            @pl.when(z < lines - 1)
            def _():
                send_copy(z - s, h, place(z - s, h), right_s, col).wait_send()

        @pl.when(z + s < lines)
        def _():
            mate_copy(z + s, h, place(z + s, h)).wait_send()

            @pl.when(z > 0)
            def _():
                send_copy(z + s, h, place(z + s, h), left_s, col).wait_send()


def body(n_row, n_col, panel, trailing, counts):
    width = panel.shape[1]
    rows, columns = bits_of("row", n_row), bits_of("col", n_col)
    packed_rows = len(blocks_of(width)) * LANES
    fold = two_streams(packed_rows, rows + columns, rows + columns)
    total = two_streams(width, rows, rows)
    chunks = n_col // CORES * HALVES
    vmem = lambda *shape: pltpu.VMEM(shape, jnp.float32)
    dma = lambda n: pltpu.SemaphoreType.DMA((n,))
    spans = trailing.shape[1]
    return pl.pallas_call(
        functools.partial(kernel, n_row, n_col),
        out_shape=(
            jax.ShapeDtypeStruct((width, width), jnp.float32),
            jax.ShapeDtypeStruct((width, spans), jnp.float32),
        ),
        in_specs=[
            pl.BlockSpec(memory_space=pltpu.SMEM),
            pl.BlockSpec(memory_space=pltpu.VMEM),
            pl.BlockSpec(memory_space=pl.ANY),
        ],
        out_specs=[pl.BlockSpec(memory_space=pltpu.VMEM)] * 2,
        scratch_shapes=[
            vmem(packed_rows, LANES), vmem(packed_rows, LANES),
            vmem(landing_rows(fold), LANES),
            dma(4 * len(rows + columns)), dma(4 * len(rows + columns)),
            vmem(*(n_col * panel.shape[0], width)), vmem(*trailing.shape),
            vmem(width, spans), vmem(width, spans), vmem(landing_rows(total), spans),
            dma(4 * len(rows)), dma(4 * len(rows)),
            vmem(width, 2 * width), vmem(LANES, 2 * LANES),
            pltpu.SemaphoreType.DMA,
            dma(chunks), dma(chunks), dma(chunks), dma(chunks), dma(chunks),
        ],
        compiler_params=pltpu.CompilerParams(
            collective_id=0, has_side_effects=True, vmem_limit_bytes=56 * 2**20
        ),
    )(counts, panel, trailing)


def solution(mesh):
    return jax.shard_map(
        functools.partial(body, mesh.shape["row"], mesh.shape["col"]),
        mesh=mesh,
        in_specs=(P(("row", "col"), None), P("row", "col"), P("row")),
        out_specs=(P(), P(None, "col")),
        check_vma=False,
    )
```
